32 devices in a mesh: dp: 4 (over z), row: 2 (over x), col: 4 (over y, core).
Axes of the slice: x: 2, y: 2, z: 4, core: 2. Of those that a mesh axis runs over, the one named last changes fastest.
Arguments:
- block_input: bfloat16 [8192, 1536], P('dp', 'row'), may hold values from -16 to 16
- positions: int32 [8192], P('dp'), may hold values from 0 to 511, as said below
- attn_gain: float32 [1536], P('row'), may hold values from 0.5 to 1.5
- w_qkv: bfloat16 [1536, 3072], P('row', 'col'), may hold values from -1.04613624 to 1.04613624
- w_out: bfloat16 [1536, 1536], P('col', 'row'), may hold values from -1.25 to 1.25
- ffn_gain: float32 [1536], P('row'), may hold values from 0.5 to 1.5
- w_gate: bfloat16 [1536, 4096], P('row', 'col'), may hold values from -0.15625 to 0.15625
- w_up: bfloat16 [1536, 4096], P('row', 'col'), may hold values from -0.15625 to 0.15625
- w_down: bfloat16 [4096, 1536], P('col', 'row'), may hold values from -0.09375 to 0.09375
- out_grad: bfloat16 [8192, 1536], P('dp', 'row'), may hold values from -6 to 6
Outputs:
- block_output: bfloat16 [8192, 1536], P('dp', 'row')
- input_grad: bfloat16 [8192, 1536], P('dp', 'row')
- attn_gain_grad: float32 [1536], P('row')
- w_qkv_grad: float32 [1536, 3072], P('row', 'col')
- w_out_grad: float32 [1536, 1536], P('col', 'row')
- ffn_gain_grad: float32 [1536], P('row')
- w_gate_grad: float32 [1536, 4096], P('row', 'col')
- w_up_grad: float32 [1536, 4096], P('row', 'col')
- w_down_grad: float32 [4096, 1536], P('col', 'row')
The draws below stay inside these ranges and needn't reach their ends.
Inputs may be any that keep to these rules, and one draw needn't show every extreme that they name: `positions`: each sequence of 512 tokens holds one to five packed documents; a token's position counts from the first token of its document; some sequence is a single document.
All inputs are finite; a program needn't handle non-finite values.
Results may differ from the reference program's by a relative error of at most 0.015.
Values may be sent and summed in bfloat16 or wider, within the bound.
A program may use at most 192 MiB of HBM per device.

```python
import math
import jax
import jax.numpy as jnp
from jax import lax

D = 1536
H = 16
KV = 8
HD = 96
FF = 4096
SEQ_LEN = 512
QKV = 3072
TOKENS = 8192


def draw_block_input(key, part):
    first, second = jax.random.split(key, 2)
    column = jnp.arange(D).astype(jnp.float32) / D
    rough = jax.random.uniform(second, (D,), jnp.float32, 0.7, 1.4)
    col_scale = 0.6 * jnp.exp(math.log(3.0) * column) * rough
    values = jax.random.truncated_normal(first, -6.0, 6.0, (TOKENS, D), jnp.float32) * col_scale
    return values.astype(jnp.bfloat16)


def draw_positions(key, part):
    count = TOKENS // SEQ_LEN
    first, second = jax.random.split(key)
    cuts = jax.random.randint(first, (count, 4), 1, SEQ_LEN)
    chosen = jax.random.randint(second, (), 0, count)
    index = jnp.arange(SEQ_LEN).astype(jnp.int32)
    marks = jnp.any(index[None, :, None] == cuts[:, None, :], axis=2)
    marks = jnp.logical_and(marks, (jnp.arange(count) != chosen)[:, None])
    begins = lax.cummax(jnp.where(marks, index[None, :], 0), axis=1)
    return (index[None, :] - begins).reshape(-1).astype(jnp.int32)


def draw_w_qkv(key, part):
    sigma = D ** (-0.5)
    group = H // KV
    base = jax.random.truncated_normal(key, -6.0, 6.0, (D, KV, group + 2, HD), jnp.float32) * sigma
    return base.reshape(D, (H + 2 * KV) * HD).astype(jnp.bfloat16)


def levels(key, dims, cuts, smallest, high):
    def one(axis_at, shards_of):
        steps = jax.random.uniform(jax.random.fold_in(jax.random.fold_in(key, 6), axis_at), (shards_of,), jnp.float32, smallest / len(cuts), high / len(cuts))
        return jnp.repeat(jnp.exp(steps), dims[axis_at] // shards_of).reshape((-1,) + (1,) * (len(dims) - axis_at - 1))

    level = one(*cuts[0])
    for cut in cuts[1:]:
        level = level * one(*cut)
    return level


def bell_draw(stream_key, dims, scale, limit, cuts=(), dtype=jnp.bfloat16):
    gain = levels(stream_key, dims, cuts, -0.22, 0.18) if cuts else 1.0
    array = jax.random.normal(stream_key, dims, jnp.float32) * scale * gain
    return jnp.minimum(jnp.maximum(array, -limit), limit).astype(dtype)


def setup_inputs(seed: int = 0) -> dict:
    splits = jax.random.split(jax.random.key(seed), 11)
    block_input = draw_block_input(jax.random.fold_in(splits[10], 71), 0)
    positions = draw_positions(jax.random.fold_in(splits[10], 71), 0)
    attn_gain = jnp.clip(1.0 + 0.1 * jax.random.normal(splits[2], (D,), jnp.float32), 0.5, 1.5)
    w_qkv = draw_w_qkv(jax.random.fold_in(splits[10], 71), 0)
    w_out = bell_draw(splits[4], (H * HD, D), (H * HD // 64) ** -0.5, 1.25, ((0, 4), (1, 2)))
    ffn_gain = jnp.clip(1.0 + 0.1 * jax.random.normal(splits[5], (D,), jnp.float32), 0.5, 1.5)
    w_gate = bell_draw(splits[6], (D, FF), D ** -0.5, 0.15625, ((0, 2), (1, 4)))
    w_up = bell_draw(splits[7], (D, FF), D ** -0.5, 0.15625, ((0, 2), (1, 4)))
    w_down = bell_draw(splits[8], (FF, D), FF ** -0.5, 0.09375, ((0, 4), (1, 2)))
    out_grad = bell_draw(splits[9], (TOKENS, D), 1.0, 6.0, ((0, 4), (1, 2)))
    return {"block_input": block_input, "positions": positions, "attn_gain": attn_gain, "w_qkv": w_qkv, "w_out": w_out, "ffn_gain": ffn_gain, "w_gate": w_gate, "w_up": w_up, "w_down": w_down, "out_grad": out_grad}


EPS = 1e-05
THETA = 100000.0

def rotate(values, cosine, sine, sign):
    half = values.shape[-1] // 2
    first = values[..., :half]
    second = values[..., half:]
    return jnp.concatenate([first * cosine - sign * second * sine, second * cosine + sign * first * sine], axis=-1)

def angle_tables(pos):
    freqs = THETA ** (-(jnp.arange(0, HD, 2).astype(jnp.float32) / HD))
    angles = pos.astype(jnp.float32)[..., None] * freqs
    return (jnp.cos(angles), jnp.sin(angles))

def one_sequence(xin, pos, dy, attn_gain, w_qkv, w_out, ffn_gain, w_gate, w_up, w_down):
    f32 = jnp.float32
    bf = jnp.bfloat16
    group = H // KV
    scale = HD ** (-0.5)
    xf = xin.astype(f32)
    inv1 = lax.rsqrt(lax.optimization_barrier(jnp.mean(xf * xf, axis=1, keepdims=True)) + EPS)
    normed1 = (xf * inv1 * attn_gain).astype(bf)
    qkv = jnp.dot(normed1, w_qkv, preferred_element_type=f32).reshape(SEQ_LEN, KV, group + 2, HD)
    cosine, sine = angle_tables(pos)
    cq = cosine[:, None, None, :]
    sq = sine[:, None, None, :]
    ck = cosine[:, None, :]
    sk = sine[:, None, :]
    queries = rotate(qkv[:, :, :group], cq, sq, 1.0).astype(bf)
    keys = rotate(qkv[:, :, group], ck, sk, 1.0).astype(bf)
    vals = qkv[:, :, group + 1].astype(bf)
    qf = queries.astype(f32)
    kf = keys.astype(f32)
    vf = vals.astype(f32)
    causal = jnp.arange(SEQ_LEN)[:, None] >= jnp.arange(SEQ_LEN)[None, :]
    scores = jnp.einsum('ikph,jkh->kpij', qf, kf) * scale
    scores = jnp.where(causal, scores, -1e+30)
    top = lax.optimization_barrier(jnp.max(scores, axis=-1, keepdims=True))
    lse = top + jnp.log(lax.optimization_barrier(jnp.sum(jnp.exp(scores - top), axis=-1, keepdims=True)))
    probs = jnp.exp(scores - lse)
    probs_b = probs.astype(bf).astype(f32)
    mixed = jnp.einsum('kpij,jkh->ikph', probs_b, vf).astype(bf)
    attn_rows = mixed.reshape(SEQ_LEN, H * HD)
    hidden = xf + jnp.dot(attn_rows, w_out, preferred_element_type=f32)
    inv2 = lax.rsqrt(lax.optimization_barrier(jnp.mean(hidden * hidden, axis=1, keepdims=True)) + EPS)
    normed2 = (hidden * inv2 * ffn_gain).astype(bf)
    gate = jnp.dot(normed2, w_gate, preferred_element_type=f32)
    up = jnp.dot(normed2, w_up, preferred_element_type=f32)
    act = (jax.nn.silu(gate) * up).astype(bf)
    output = (hidden + jnp.dot(act, w_down, preferred_element_type=f32)).astype(bf)
    dyf = dy.astype(f32)
    w_down_grad = jnp.dot(act.T, dy, preferred_element_type=f32)
    act_grad = jnp.dot(dy, w_down.T, preferred_element_type=f32)
    sig = jax.nn.sigmoid(gate)
    gate_grad = (act_grad * up * sig * (1.0 + gate * (1.0 - sig))).astype(bf)
    up_grad = (act_grad * gate * sig).astype(bf)
    w_gate_grad = jnp.dot(normed2.T, gate_grad, preferred_element_type=f32)
    w_up_grad = jnp.dot(normed2.T, up_grad, preferred_element_type=f32)
    normed2_grad = jnp.dot(gate_grad, w_gate.T, preferred_element_type=f32) + jnp.dot(up_grad, w_up.T, preferred_element_type=f32)
    ffn_gain_grad = lax.optimization_barrier(jnp.sum(normed2_grad * hidden * inv2, axis=0))
    scaled2 = normed2_grad * ffn_gain
    hidden_grad = dyf + inv2 * (scaled2 - hidden * inv2 * inv2 * lax.optimization_barrier(jnp.mean(scaled2 * hidden, axis=1, keepdims=True)))
    hidden_b = hidden_grad.astype(bf)
    w_out_grad = jnp.dot(attn_rows.T, hidden_b, preferred_element_type=f32)
    mixed_grad = jnp.dot(hidden_b, w_out.T, preferred_element_type=f32).astype(bf).reshape(SEQ_LEN, KV, group, HD)
    mgf = mixed_grad.astype(f32)
    value_grad = jnp.einsum('kpij,ikph->jkh', probs_b, mgf)
    prob_grad = jnp.einsum('ikph,jkh->kpij', mgf, vf)
    delta = jnp.transpose(lax.optimization_barrier(jnp.sum(mgf * mixed.astype(f32), axis=-1)), (1, 2, 0))[..., None]
    score_grad = (probs * (prob_grad - delta)).astype(bf).astype(f32)
    query_grad = rotate(jnp.einsum('kpij,jkh->ikph', score_grad, kf) * scale, cq, sq, -1.0)
    key_grad = rotate(jnp.einsum('kpij,ikph->jkh', score_grad, qf) * scale, ck, sk, -1.0)
    qkv_grad = jnp.concatenate([query_grad, key_grad[:, :, None], value_grad[:, :, None]], axis=2).astype(bf).reshape(SEQ_LEN, QKV)
    w_qkv_grad = jnp.dot(normed1.T, qkv_grad, preferred_element_type=f32)
    normed1_grad = jnp.dot(qkv_grad, w_qkv.T, preferred_element_type=f32)
    attn_gain_grad = lax.optimization_barrier(jnp.sum(normed1_grad * xf * inv1, axis=0))
    scaled1 = normed1_grad * attn_gain
    input_grad = (hidden_grad + inv1 * (scaled1 - xf * inv1 * inv1 * lax.optimization_barrier(jnp.mean(scaled1 * xf, axis=1, keepdims=True)))).astype(bf)
    grads = (attn_gain_grad, w_qkv_grad, w_out_grad, ffn_gain_grad, w_gate_grad, w_up_grad, w_down_grad)
    return (output, input_grad, grads)

def reference(block_input, positions, attn_gain, w_qkv, w_out, ffn_gain, w_gate, w_up, w_down, out_grad):
    count = block_input.shape[0] // SEQ_LEN
    items = (block_input.reshape(count, SEQ_LEN, D), positions.reshape(count, SEQ_LEN), out_grad.reshape(count, SEQ_LEN, D))
    start = (jnp.zeros((D,), jnp.float32), jnp.zeros((D, QKV), jnp.float32), jnp.zeros((H * HD, D), jnp.float32), jnp.zeros((D,), jnp.float32), jnp.zeros((D, FF), jnp.float32), jnp.zeros((D, FF), jnp.float32), jnp.zeros((FF, D), jnp.float32))

    def step(carry, item):
        output, input_grad, grads = one_sequence(item[0], item[1], item[2], attn_gain, w_qkv, w_out, ffn_gain, w_gate, w_up, w_down)
        return (tuple((total + part for total, part in zip(carry, grads))), (output, input_grad))
    totals, stacked = lax.scan(step, start, items)
    block_output = stacked[0].reshape(count * SEQ_LEN, D)
    input_grad = stacked[1].reshape(count * SEQ_LEN, D)
    return (block_output, input_grad, totals[0], totals[1], totals[2], totals[3], totals[4], totals[5], totals[6])
```

```python
import jax
import jax.numpy as jnp
from jax import lax
from jax.experimental import pallas as pl
from jax.experimental.pallas import tpu as pltpu
from jax.sharding import PartitionSpec as P

HD = 96
GROUP = 2
SEQ_LEN = 512
EPS = 1e-05
THETA = 100000.0
MESH = pl.DeviceIdType.MESH
f32 = jnp.float32
bf = jnp.bfloat16


class Net:
    def __init__(self, send_sem, recv_sem, row=True, col=True):
        self.row, self.col = lax.axis_index("row"), lax.axis_index("col")
        self.core = lax.rem(self.col, 2)
        self.y = self.col // 2
        self.far = lax.rem(self.col + 2, 4)
        self.px = {"row": 1 - self.row}
        self.py = {"col": self.far}
        self.pc = {"col": 2 * self.y + 1 - self.core}
        self.send_sem, self.recv_sem, self.n = send_sem, recv_sem, 0
        self.copies = []
        barrier = pltpu.get_barrier_semaphore()
        partners = ([self.px] if row else []) + ([self.py, self.pc] if col else [])
        for partner in partners:
            pl.semaphore_signal(barrier, inc=1, device_id=partner, device_id_type=MESH)
        pl.semaphore_wait(barrier, len(partners))

    def send(self, src, dst, partner):
        copy = pltpu.make_async_remote_copy(
            src_ref=src,
            dst_ref=dst,
            send_sem=self.send_sem.at[self.n],
            recv_sem=self.recv_sem.at[self.n],
            device_id=partner,
            device_id_type=MESH,
        )
        self.n += 1
        copy.start()
        self.copies.append(copy)
        return copy

    def drain(self):
        for copy in self.copies:
            copy.wait_send()


def ds(start, size, unit):
    return pl.ds(pl.multiple_of(start, unit), size)


def comm_call(kernel, outs, scratch, copies, cid, *args, local=0, nbytes=0, any_in=False):
    vm = pl.BlockSpec(memory_space=pltpu.VMEM)
    sems = [pltpu.SemaphoreType.DMA((copies,)), pltpu.SemaphoreType.DMA((copies,))]
    if local:
        sems.append(pltpu.SemaphoreType.DMA((local,)))
    return pl.pallas_call(
        kernel,
        out_shape=outs,
        in_specs=[pl.BlockSpec(memory_space=pl.ANY) if any_in else vm] * len(args),
        out_specs=[vm] * len(outs),
        scratch_shapes=scratch + sems,
        compiler_params=pltpu.CompilerParams(
            collective_id=cid, has_side_effects=True, vmem_limit_bytes=56 * 2**20
        ),
        cost_estimate=pl.CostEstimate(flops=0, bytes_accessed=nbytes, transcendentals=0),
    )(*args)


def fetch_kernel(x_ref, dy_ref, xo, dyo, ssem, rsem, lsem):
    net = Net(ssem, rsem)
    rows, wide = x_ref.shape
    part = rows // 2
    block = part // 4
    own, peer = net.row * wide, (1 - net.row) * wide
    streams = [
        (x_ref, (1 - net.row) * part, xo, 0),
        (dy_ref, 0, dyo, 0),
        (dy_ref, part, dyo, part),
    ]
    first = [
        net.send(
            src.at[ds(sb + net.col * block, block, 16), :],
            out.at[ds(db + net.col * block, block, 16), ds(own, wide, 128)],
            net.px,
        )
        for src, sb, out, db in streams
    ]
    local = [
        pltpu.make_async_copy(
            x_ref.at[ds(net.row * part, part, 16), :], xo.at[:, ds(own, wide, 128)], lsem.at[0]
        ),
        pltpu.make_async_copy(dy_ref, dyo.at[:, ds(own, wide, 128)], lsem.at[1]),
    ]
    for copy in local:
        copy.start()

    def spot(stream, col):
        return stream[2].at[ds(stream[3] + col * block, block, 16), ds(peer, wide, 128)]

    over_y, over_c = [], []
    for stream, copy in zip(streams, first):
        copy.wait_recv()
        here = spot(stream, net.col)
        over_y.append(net.send(here, here, net.py))
        over_c.append(net.send(here, here, net.pc))
    for stream, copy in zip(streams, over_y):
        copy.wait_recv()
        there = spot(stream, net.far)
        over_c.append(net.send(there, there, net.pc))
    for copy in over_c:
        copy.wait_recv()
    for copy in local:
        copy.wait()
    net.drain()


def fetch(x, dy):
    rows, wide = x.shape
    return comm_call(
        fetch_kernel,
        [
            jax.ShapeDtypeStruct((rows // 2, 2 * wide), x.dtype),
            jax.ShapeDtypeStruct((rows, 2 * wide), dy.dtype),
        ],
        [],
        12,
        1,
        x,
        dy,
        local=2,
        nbytes=4 * x.size * 6,
        any_in=True,
    )


def spread_kernel(h_ref, out, ssem, rsem, lsem):
    net = Net(ssem, rsem)
    block, wide = h_ref.shape[0], h_ref.shape[1] // 2
    part = out.shape[0] // 2
    own, peer = net.row * wide, (1 - net.row) * wide

    def spot(row, col):
        return out.at[ds(row * part + col * block, block, 16), :]

    mine = spot(net.row, net.col)
    over_x = net.send(h_ref.at[:, ds(peer, wide, 128)], mine, net.px)
    half = h_ref.at[:, ds(own, wide, 128)]
    over_y = [net.send(half, mine, net.py)]
    over_c = [net.send(half, mine, net.pc)]
    local = pltpu.make_async_copy(half, mine, lsem.at[0])
    local.start()
    over_x.wait_recv()
    theirs = spot(1 - net.row, net.col)
    over_y.append(net.send(theirs, theirs, net.py))
    over_c.append(net.send(theirs, theirs, net.pc))
    for row, copy in zip((net.row, 1 - net.row), over_y):
        copy.wait_recv()
        there = spot(row, net.far)
        over_c.append(net.send(there, there, net.pc))
    for copy in over_c:
        copy.wait_recv()
    local.wait()
    net.drain()


def spread(h, rows):
    return comm_call(
        spread_kernel,
        [jax.ShapeDtypeStruct((rows, h.shape[1] // 2), h.dtype)],
        [],
        7,
        2,
        h,
        local=1,
        nbytes=rows * h.shape[1] * 8,
    )[0]


def gather_col_kernel(h_ref, out, ssem, rsem, lsem):
    net = Net(ssem, rsem, row=False)
    block = h_ref.shape[0]

    def spot(col):
        return out.at[ds(col * block, block, 16), :]

    mine = spot(net.col)
    over_y = net.send(h_ref, mine, net.py)
    over_c = [net.send(h_ref, mine, net.pc)]
    local = pltpu.make_async_copy(h_ref, mine, lsem.at[0])
    local.start()
    over_y.wait_recv()
    there = spot(net.far)
    over_c.append(net.send(there, there, net.pc))
    for copy in over_c:
        copy.wait_recv()
    local.wait()
    net.drain()


def gather_col(h):
    return comm_call(
        gather_col_kernel,
        [jax.ShapeDtypeStruct((4 * h.shape[0], h.shape[1]), h.dtype)],
        [],
        3,
        3,
        h,
        local=1,
        nbytes=h.size * 24,
    )[0]


def add_rows(dst, terms, rows):
    step = 32

    def one(i, carry):
        at = pl.multiple_of(i * step, step)
        total = None
        for ref, base in terms:
            piece = ref[pl.ds(pl.multiple_of(base + at, 16), step), :].astype(f32)
            total = piece if total is None else total + piece
        ref, base = dst
        ref[pl.ds(pl.multiple_of(base + at, 16), step), :] = total.astype(ref.dtype)
        return carry

    lax.fori_loop(0, rows // step, one, 0)


def reduce_col_kernel(p_ref, out, near, mid, far, ssem, rsem):
    net = Net(ssem, rsem, row=False)
    rows = p_ref.shape[0] // 4
    pieces = 2
    size = rows // pieces
    over_c = []
    for y in (1 - net.y, net.y):
        for i in range(pieces):
            n = len(over_c)
            base = (2 * y + 1 - net.core) * rows + i * size
            over_c.append(
                net.send(p_ref.at[ds(base, size, 16), :], near.at[pl.ds(n * size, size), :], net.pc)
            )
    over_y = []
    for i in range(pieces):
        over_c[i].wait_recv()
        base = net.far * rows + i * size
        add_rows((mid, i * size), [(p_ref, base), (near, i * size)], size)
        here = pl.ds(i * size, size)
        over_y.append(net.send(mid.at[here, :], far.at[here, :], net.py))
    for i in range(pieces):
        over_c[pieces + i].wait_recv()
    for i in range(pieces):
        over_y[i].wait_recv()
        base = net.col * rows + i * size
        add_rows(
            (out, i * size),
            [(p_ref, base), (near, rows + i * size), (far, i * size)],
            size,
        )
    net.drain()


def reduce_col(p):
    rows, wide = p.shape[0] // 4, p.shape[1]
    return comm_call(
        reduce_col_kernel,
        [jax.ShapeDtypeStruct((rows, wide), f32)],
        [
            pltpu.VMEM((2 * rows, wide), p.dtype),
            pltpu.VMEM((rows, wide), p.dtype),
            pltpu.VMEM((rows, wide), p.dtype),
        ],
        6,
        4,
        p,
        nbytes=p.size * 6,
    )[0]


def gather_all_kernel(h_ref, out, ssem, rsem, lsem):
    net = Net(ssem, rsem)
    block = h_ref.shape[0]
    half = block // 2

    def spot(row, col, part):
        return out.at[ds((row * 4 + col) * block + part * half, half, 16), :]

    a, b = h_ref.at[pl.ds(0, half), :], h_ref.at[pl.ds(half, half), :]
    mine_a, mine_b = spot(net.row, net.col, 0), spot(net.row, net.col, 1)
    y_a = net.send(a, mine_a, net.py)
    x_b = net.send(b, mine_b, net.px)
    x_a = net.send(a, mine_a, net.px)
    y_b = net.send(b, mine_b, net.py)
    over_c = [net.send(a, mine_a, net.pc), net.send(b, mine_b, net.pc)]
    local = pltpu.make_async_copy(
        h_ref, out.at[ds((net.row * 4 + net.col) * block, block, 16), :], lsem.at[0]
    )
    local.start()
    y_a.wait_recv()
    got = spot(net.row, net.far, 0)
    x_ya = net.send(got, got, net.px)
    over_c.append(net.send(got, got, net.pc))
    x_b.wait_recv()
    got = spot(1 - net.row, net.col, 1)
    y_xb = net.send(got, got, net.py)
    over_c.append(net.send(got, got, net.pc))
    for copy, row, col, part in (
        (x_a, 1 - net.row, net.col, 0),
        (y_b, net.row, net.far, 1),
        (x_ya, 1 - net.row, net.far, 0),
        (y_xb, 1 - net.row, net.far, 1),
    ):
        copy.wait_recv()
        got = spot(row, col, part)
        over_c.append(net.send(got, got, net.pc))
    for copy in over_c:
        copy.wait_recv()
    local.wait()
    net.drain()


def gather_all(h):
    return comm_call(
        gather_all_kernel,
        [jax.ShapeDtypeStruct((8 * h.shape[0], h.shape[1]), h.dtype)],
        [],
        14,
        5,
        h,
        local=1,
        nbytes=h.size * 40,
    )[0]


def reduce_all_kernel(p_ref, out, near, mid, far, ssem, rsem):
    net = Net(ssem, rsem)
    block = p_ref.shape[0] // 8
    half = block // 2
    nx, ny = 1 - net.row, 1 - net.y
    order = [
        (nx, ny, 0),
        (nx, ny, 1),
        (nx, net.y, 0),
        (net.row, ny, 1),
        (net.row, ny, 0),
        (nx, net.y, 1),
        (net.row, net.y, 0),
        (net.row, net.y, 1),
    ]

    def base(i, core):
        x, y, part = order[i]
        return (x * 4 + 2 * y + core) * block + part * half

    def at(i):
        return pl.ds(i * half, half)

    over_c = [
        net.send(p_ref.at[ds(base(i, 1 - net.core), half, 16), :], near.at[at(i), :], net.pc)
        for i in range(8)
    ]
    sent = []
    for i in range(6):
        over_c[i].wait_recv()
        terms = [(p_ref, base(i, net.core)), (near, i * half)]
        if i >= 4:
            sent[i - 4].wait_recv()
            terms.append((far, (i - 4) * half))
        add_rows((mid, i * half), terms, half)
        sent.append(
            net.send(mid.at[at(i), :], far.at[at(i), :], net.px if i in (0, 2, 5) else net.py)
        )
    for i in (6, 7):
        over_c[i].wait_recv()
        sent[i - 4].wait_recv()
        sent[i - 2].wait_recv()
        add_rows(
            (out, (i - 6) * half),
            [
                (p_ref, base(i, net.core)),
                (near, i * half),
                (far, (i - 4) * half),
                (far, (i - 2) * half),
            ],
            half,
        )
    net.drain()


def reduce_all(p):
    rows, wide = p.shape[0] // 8, p.shape[1]
    return comm_call(
        reduce_all_kernel,
        [jax.ShapeDtypeStruct((rows, wide), f32)],
        [
            pltpu.VMEM((4 * rows, wide), p.dtype),
            pltpu.VMEM((3 * rows, wide), p.dtype),
            pltpu.VMEM((3 * rows, wide), p.dtype),
        ],
        14,
        6,
        p,
        nbytes=p.size * 6,
    )[0]


def rotate(values, cosine, sine, sign):
    half = values.shape[-1] // 2
    first = values[..., :half]
    second = values[..., half:]
    return jnp.concatenate(
        [first * cosine - sign * second * sine, second * cosine + sign * first * sine], axis=-1
    )


def angle_tables(pos):
    freqs = THETA ** (-(jnp.arange(0, HD, 2).astype(jnp.float32) / HD))
    angles = pos.astype(jnp.float32)[..., None] * freqs
    return (jnp.cos(angles), jnp.sin(angles))


def dot(left, right, lhs, rhs, out=f32):
    return lax.dot_general(
        left, right, (((lhs,), (rhs,)), ((), ())), preferred_element_type=f32
    ).astype(out)


def swap(values):
    return lax.ppermute(values, "row", [(0, 1), (1, 0)])


def in_order(row, own, peer, axis):
    return jnp.where(
        row == 0,
        jnp.concatenate([own, peer], axis=axis),
        jnp.concatenate([peer, own], axis=axis),
    )


def half_of(values, index, axis):
    size = values.shape[axis] // 2
    return lax.dynamic_slice_in_dim(values, index * size, size, axis)


def body(block_input, positions, attn_gain, w_qkv, w_out, ffn_gain, w_gate, w_up, w_down, out_grad):
    row, col = lax.axis_index("row"), lax.axis_index("col")
    n_dp = lax.axis_size("dp")
    rows_all, half_wide = block_input.shape
    rows_half = rows_all // 2
    rows_own = rows_half // 4
    wide = 2 * half_wide
    kv_local = w_qkv.shape[1] // ((GROUP + 2) * HD)
    seqs = rows_half // SEQ_LEN
    scale = HD ** (-0.5)

    gains = jnp.stack([attn_gain, ffn_gain])
    gains_peer = swap(gains)
    wq_peer = swap(w_qkv)
    x_rows, dy_all = fetch(block_input, out_grad)
    w_out_l, w_gate_l, w_up_l, w_down_l, wq_peer = lax.optimization_barrier(
        (w_out, w_gate, w_up, w_down, wq_peer)
    )
    gains_all = in_order(row, gains, gains_peer, 1)
    g1, g2 = gains_all[0], gains_all[1]
    wq = in_order(row, w_qkv, wq_peer, 0)
    wo = in_order(row, w_out_l, swap(w_out_l), 1)
    gu = jnp.stack([w_gate_l, w_up_l], axis=1)
    units = gu.shape[2] // 2
    gu_mine = half_of(gu, row, 2).reshape(half_wide, 2 * units)
    gu_theirs = half_of(gu, 1 - row, 2).reshape(half_wide, 2 * units)
    wgu = in_order(row, gu_mine, swap(gu_theirs), 0)
    wd = in_order(row, half_of(w_down_l, row, 0), swap(half_of(w_down_l, 1 - row, 0)), 1)

    xf = x_rows.astype(f32)
    inv1 = lax.rsqrt(jnp.sum(xf * xf, axis=1, keepdims=True) / wide + EPS)
    normed1 = (xf * inv1 * g1).astype(bf)
    qkv = dot(normed1, wq, 1, 0)
    grouped = qkv.reshape(seqs, SEQ_LEN, kv_local, GROUP + 2, HD)
    pos = half_of(positions, row, 0).reshape(seqs, SEQ_LEN)
    cosine, sine = angle_tables(pos)
    cq = cosine[:, :, None, None, :]
    sq = sine[:, :, None, None, :]
    ck = cosine[:, :, None, :]
    sk = sine[:, :, None, :]
    queries = rotate(grouped[:, :, :, :GROUP], cq, sq, 1.0).astype(bf)
    keys = rotate(grouped[:, :, :, GROUP], ck, sk, 1.0).astype(bf)
    vals = grouped[:, :, :, GROUP + 1].astype(bf)
    causal = jnp.arange(SEQ_LEN)[:, None] >= jnp.arange(SEQ_LEN)[None, :]
    scores = jnp.einsum("sikph,sjkh->skpij", queries, keys, preferred_element_type=f32) * scale
    scores = jnp.where(causal, scores, -1e30)
    top = jnp.max(scores, axis=-1, keepdims=True)
    lse = top + jnp.log(jnp.sum(jnp.exp(scores - top), axis=-1, keepdims=True))
    probs_b = jnp.exp(scores - lse).astype(bf)
    mixed = jnp.einsum("skpij,sjkh->sikph", probs_b, vals, preferred_element_type=f32).astype(bf)
    attn_rows = mixed.reshape(rows_half, kv_local * GROUP * HD)

    x_own = lax.dynamic_slice_in_dim(x_rows, col * rows_own, rows_own, 0).astype(f32)
    inv1_own = lax.dynamic_slice_in_dim(inv1, col * rows_own, rows_own, 0)
    hidden = x_own + reduce_col(dot(attn_rows, wo, 1, 0, bf))
    inv2 = lax.rsqrt(jnp.sum(hidden * hidden, axis=1, keepdims=True) / wide + EPS)
    normed2 = gather_all((hidden * inv2 * g2).astype(bf))

    both = dot(normed2, wgu, 1, 0)
    gate, up = both[:, :units], both[:, units:]
    sig = jax.nn.sigmoid(gate)
    act = (gate * sig * up).astype(bf)
    down_part = dot(act, wd, 1, 0, bf)
    act_grad = dot(dy_all, wd, 1, 1)
    gate_grad = (act_grad * up * sig * (1.0 + gate * (1.0 - sig))).astype(bf)
    up_grad = (act_grad * gate * sig).astype(bf)
    both_grad = jnp.concatenate([gate_grad, up_grad], axis=1)
    wd_grad = dot(act, dy_all, 0, 0, bf).reshape(n_dp, units // n_dp, wide)
    wd_grad = lax.psum_scatter(wd_grad, "dp", scatter_dimension=0)
    wgu_grad = dot(normed2, both_grad, 0, 0, bf)
    wgu_grad = wgu_grad.reshape(2, n_dp, half_wide // n_dp, 2 * units).transpose(1, 0, 2, 3)
    wgu_grad = wgu_grad.reshape(n_dp, wide // n_dp, 2 * units)
    wgu_grad = lax.psum_scatter(wgu_grad, "dp", scatter_dimension=0)
    wgu_grad = wgu_grad.reshape(2, half_wide // n_dp, 2 * units)
    n2_grad = reduce_all(dot(both_grad, wgu, 1, 1, bf))
    block_own = (hidden + reduce_all(down_part)).astype(bf)
    block_output = spread(block_own, rows_all)

    wd_sent = swap(half_of(wd_grad, 1 - row, 1))
    wd_pair = in_order(row, half_of(wd_grad, row, 1)[None], wd_sent[None], 0)
    wd_full = lax.all_gather(wd_pair, "dp", axis=0)
    w_down_grad = wd_full.transpose(1, 0, 2, 3).reshape(2 * units, half_wide).astype(f32)
    wgu_sent = swap(lax.dynamic_index_in_dim(wgu_grad, 1 - row, 0))
    wgu_pair = in_order(row, lax.dynamic_index_in_dim(wgu_grad, row, 0), wgu_sent, 0)
    wgu_full = lax.all_gather(wgu_pair, "dp", axis=0)
    wgu_full = wgu_full.reshape(n_dp, 2, half_wide // n_dp, 2, units).transpose(3, 0, 2, 1, 4)
    wgu_full = wgu_full.reshape(2, half_wide, 2 * units).astype(f32)
    w_gate_grad, w_up_grad = wgu_full[0], wgu_full[1]

    ffn_gain_grad = jnp.sum(n2_grad * hidden * inv2, axis=0)
    scaled2 = n2_grad * g2
    hidden_grad = lax.dynamic_slice_in_dim(
        dy_all, (row * 4 + col) * rows_own, rows_own, 0
    ).astype(f32) + inv2 * (
        scaled2
        - hidden * inv2 * inv2 * jnp.sum(scaled2 * hidden, axis=1, keepdims=True) / wide
    )
    hidden_b = gather_col(hidden_grad.astype(bf))

    wo_grad = dot(attn_rows, hidden_b, 0, 0, bf)
    wo_grad = half_of(wo_grad, row, 1) + swap(half_of(wo_grad, 1 - row, 1))
    w_out_grad = lax.psum(wo_grad, "dp").astype(f32)
    mixed_grad = dot(hidden_b, wo, 1, 1, bf).reshape(seqs, SEQ_LEN, kv_local, GROUP, HD)
    probs = jnp.exp(scores - lse)
    value_grad = jnp.einsum("skpij,sikph->sjkh", probs_b, mixed_grad, preferred_element_type=f32)
    prob_grad = jnp.einsum("sikph,sjkh->skpij", mixed_grad, vals, preferred_element_type=f32)
    delta = jnp.sum(mixed_grad.astype(f32) * mixed.astype(f32), axis=-1)
    delta = jnp.transpose(delta, (0, 2, 3, 1))[..., None]
    score_grad = (probs * (prob_grad - delta)).astype(bf)
    query_grad = rotate(
        jnp.einsum("skpij,sjkh->sikph", score_grad, keys, preferred_element_type=f32) * scale,
        cq,
        sq,
        -1.0,
    )
    key_grad = rotate(
        jnp.einsum("skpij,sikph->sjkh", score_grad, queries, preferred_element_type=f32) * scale,
        ck,
        sk,
        -1.0,
    )
    packed = jnp.concatenate(
        [query_grad, key_grad[:, :, :, None], value_grad[:, :, :, None]], axis=3
    ).astype(bf)
    qkv_grad = packed.reshape(rows_half, w_qkv.shape[1])
    wq_grad = dot(normed1, qkv_grad, 0, 0, bf)
    wq_grad = half_of(wq_grad, row, 0) + swap(half_of(wq_grad, 1 - row, 0))
    w_qkv_grad = lax.psum(wq_grad, "dp").astype(f32)
    n1_grad = reduce_col(dot(qkv_grad, wq, 1, 1, bf))

    attn_gain_grad = jnp.sum(n1_grad * x_own * inv1_own, axis=0)
    scaled1 = n1_grad * g1
    input_own = (
        hidden_grad
        + inv1_own
        * (
            scaled1
            - x_own * inv1_own * inv1_own * jnp.sum(scaled1 * x_own, axis=1, keepdims=True) / wide
        )
    ).astype(bf)
    input_grad = spread(input_own, rows_all)
    gain_grads = lax.psum(jnp.stack([attn_gain_grad, ffn_gain_grad]), ("dp", "row", "col"))
    gain_grads = half_of(gain_grads, row, 1)
    return (
        block_output,
        input_grad,
        gain_grads[0],
        w_qkv_grad,
        w_out_grad,
        gain_grads[1],
        w_gate_grad,
        w_up_grad,
        w_down_grad,
    )


def solution(mesh):
    assert mesh.shape["row"] == 2 and mesh.shape["col"] == 4
    return jax.shard_map(
        body,
        mesh=mesh,
        in_specs=(
            P("dp", "row"),
            P("dp"),
            P("row"),
            P("row", "col"),
            P("col", "row"),
            P("row"),
            P("row", "col"),
            P("row", "col"),
            P("col", "row"),
            P("dp", "row"),
        ),
        out_specs=(
            P("dp", "row"),
            P("dp", "row"),
            P("row"),
            P("row", "col"),
            P("col", "row"),
            P("row"),
            P("row", "col"),
            P("row", "col"),
            P("col", "row"),
        ),
        check_vma=False,
    )
```
